32 devices in a mesh: groups: 1, ep: 16 (over z, y, x), hp: 2 (over core).
Axes of the slice: x: 2, y: 2, z: 4, core: 2. Of those that a mesh axis runs over, the one named last changes fastest.
Arguments:
- x_pre: bfloat16 [896, 1536], P(('groups', 'ep')), may hold values from -6 to 6
- x_dec: bfloat16 [128, 1536], P(('groups', 'ep')), may hold values from -6 to 6
- prefill_query_rows: bfloat16 [896, 2048], P(('groups', 'ep'), 'hp'), may hold values from -240 to 240
- prefill_key_values: bfloat16 [2, 896, 256], P(None, ('groups', 'ep'), 'hp'), may hold values from -6.1 to 6.1
- decode_query_rows: bfloat16 [128, 2048], P(('groups', 'ep'), 'hp'), may hold values from -240 to 240
- decode_key_values: bfloat16 [2, 128, 256], P(None, ('groups', 'ep'), 'hp'), may hold values from -6 to 6
- cache: bfloat16 [2, 128, 128, 256], P(None, ('groups', 'ep'), None, 'hp'), may hold values from -6.1 to 6.1
- cache_len: int32 [128], P(('groups', 'ep')), may hold values from 2 to 128
- sinks: float32 [32], P('hp'), may hold values from -1 to 5
- o_weight: bfloat16 [2048, 1536], P('hp', 'ep'), may hold values from -0.125 to 0.125
- norm_gain: float32 [1536], replicated, may hold values from 0.5 to 1.5
- expert_ids: int32 [1024, 4], P(('groups', 'ep')), may hold values from 0 to 7, all different within a row; in each aligned block of 64 rows (0 to 63, 64 to 127, ...) at most 48 rows name the same one
- route_logits: float32 [1024, 4], P(('groups', 'ep')), may hold values from -6 to 6
- w_gate_up: bfloat16 [16, 2, 1536, 768], P('ep', None, None, 'hp'), may hold values from -0.15625 to 0.15625
- w_down: bfloat16 [16, 768, 1536], P('ep', 'hp'), may hold values from -0.15625 to 0.15625
Outputs:
- layer_out: bfloat16 [1024, 1536], P(('groups', 'ep', 'hp'))
The draws below stay inside these ranges and needn't reach their ends.
Inputs may be any that keep to these rules, and one draw needn't show every extreme that they name: `expert_ids`: each row names 4 different experts; among the rows of one index of ep no expert is named by more than 48 rows, and in every draw some expert is named by exactly 48 rows of some index.
All inputs are finite; a program needn't handle non-finite values.
Results may differ from the reference program's by a relative error of at most 0.0065.
Values may be sent and summed in bfloat16 or wider, within the bound.
A program may use at most 64 MiB of HBM per device.

```python
import math
import jax
import jax.numpy as jnp
import numpy as np
from jax import lax

D = 1536
QUERY_HEADS = 32
LOCAL_KV_HEADS = 4
HEAD_SIZE = 64
FF = 1536
TOPK = 4
PREFILL_LOCAL = 56
DEC_DEV = 8
CACHE_POSITIONS = 128
EXPERTS = 8
PREFILL_TOKENS = 896
DECODE_COUNT = 128
TOK_DEV = 64
TOKENS = 1024
SLOT = 48
N_EP = 16


def prefill_index_pairs(key):
    base_offset = jax.random.normal(jax.random.fold_in(key, 11), (2, PREFILL_TOKENS, LOCAL_KV_HEADS * HEAD_SIZE), jnp.float32)
    return jnp.clip(base_offset, -6.1, 6.1)


def draw_prefill_key_values(key, part):
    return prefill_index_pairs(key).astype(jnp.bfloat16)


def draw_prefill_query_rows(key, part):
    base_offset = jnp.clip(jax.random.normal(jax.random.fold_in(key, 13), (PREFILL_TOKENS, QUERY_HEADS * HEAD_SIZE), jnp.float32), -6.0, 6.0)
    return jnp.clip(base_offset, -240.0, 240.0).astype(jnp.bfloat16)


def draw_cache(key, part):
    base_offset = jnp.clip(jax.random.normal(jax.random.fold_in(key, 22), (2, DECODE_COUNT, CACHE_POSITIONS, LOCAL_KV_HEADS * HEAD_SIZE), jnp.float32), -6.0, 6.0)
    return base_offset.astype(jnp.bfloat16)


def draw_decode_query_rows(key, part):
    base_offset = jnp.clip(jax.random.normal(jax.random.fold_in(key, 23), (DECODE_COUNT, QUERY_HEADS * HEAD_SIZE), jnp.float32), -6.0, 6.0)
    return jnp.clip(base_offset, -240.0, 240.0).astype(jnp.bfloat16)


def plant(values, key, smallest, top_value):
    shape = values.shape
    index_at = [jax.random.randint(jax.random.fold_in(key, axis), (), 0, shape[axis]) for axis in range(len(shape))]
    values = values.at[tuple(index_at)].set(smallest)
    longest = shape.index(max(shape))
    index_at[longest] = (index_at[longest] + 1) % shape[longest]
    return values.at[tuple(index_at)].set(top_value)


def shard_levels(stream_key, dims, pieces, least, largest):
    factor_of, own = 1.0, jax.random.fold_in(stream_key, 6)
    for axis_at, parts in pieces:
        draws = jnp.exp(jax.random.uniform(jax.random.fold_in(own, axis_at), (parts,), jnp.float32, least / len(pieces), largest / len(pieces)))
        factor_of = factor_of * jnp.repeat(draws, dims[axis_at] // parts).reshape([-1 if axis == axis_at else 1 for axis in range(len(dims))])
    return factor_of


def shared_out(key, own, number, rows, number_of, top, limit, lean):
    ranking = jax.random.permutation(key, number_of)
    heavy_load, ordinary = portions_of(number_of, rows * top, limit, lean, True), portions_of(number_of, rows * top, limit, lean, False)
    places = jnp.arange(number_of)

    def named(sizes, offset_by):
        used = int((sizes > 0).sum())
        fixed = max(1, used // 4)
        shifted = fixed + (places - fixed + offset_by * (used - fixed)) % max(1, number_of - fixed)
        return jnp.zeros((number_of,), jnp.int32).at[ranking[jnp.where(places < fixed, places, shifted)]].set(jnp.asarray(sizes, jnp.int32))

    sizes = jnp.where(number % 4 == 0, named(heavy_load, number // 4), named(ordinary, number - number // 4 - 1))
    mixed = jax.random.permutation(jax.random.fold_in(own, 3), number_of)
    giver, receiver = mixed[0:number_of // 2 * 2:2], mixed[1:number_of // 2 * 2:2]
    room = jnp.minimum(sizes[giver] - 1, limit - sizes[receiver]) // 2
    room = jnp.where((giver == ranking[0]) | (receiver == ranking[0]) | (sizes[receiver] == 0), 0, jnp.maximum(room, 0))
    shifted = jax.random.randint(jax.random.fold_in(own, 4), (number_of // 2,), 0, 1 << 20) % (room + 1)
    sizes = sizes.at[giver].add(-shifted).at[receiver].add(shifted)
    items = jnp.searchsorted(jnp.cumsum(sizes), jnp.arange(rows * top), side="right").astype(jnp.int32)
    grid = items.reshape(top, rows).T
    grid = grid[jax.random.permutation(jax.random.fold_in(own, 1), rows)]
    offset_by = jax.random.randint(jax.random.fold_in(own, 2), (rows, 1), 0, top)
    return jnp.take_along_axis(grid, (jnp.arange(top)[None, :] + offset_by) % top, axis=1)


def portions_of(number_of, total, most, skew, full):
    weights = [(1 << 20) // math.isqrt(rank ** skew) + 1 for rank in range(1, number_of + 1)]
    largest = most if full else min(most, max(-(-total // number_of), total * weights[0] // sum(weights)))
    least = 1 if total - largest >= number_of - 1 else 0
    given, spare = [largest] + [least] * (number_of - 1), total - largest - least * (number_of - 1)
    while spare > 0:
        candidates = [i for i in range(1, number_of) if given[i] < largest] or [i for i in range(1, number_of) if given[i] < most]
        whole, budget = sum([weights[i] for i in candidates]), spare
        for i in candidates:
            extra = min(most - given[i], max(1, budget * weights[i] // whole), spare)
            given[i] = given[i] + extra
            spare = spare - extra
    return np.array(given)


def centred(stream_key, extent, deviation, limit, split=(), held_as=jnp.bfloat16):
    array = deviation * jax.random.normal(stream_key, extent, jnp.float32)
    if split:
        array = array * shard_levels(stream_key, extent, split, -0.22, 0.18)
    return jnp.clip(array, -limit, limit).astype(held_as)


def setup_inputs(seed: int = 0, part: int = 0) -> dict:
    streams_of = jax.random.split(jax.random.key(seed), 16)
    part_keys = jax.random.split(jax.random.fold_in(streams_of[15], part), 16)
    x_pre = centred(part_keys[0], (PREFILL_TOKENS, D), 1.0, 6.0, ((0, 16),))
    x_dec = centred(part_keys[1], (DECODE_COUNT, D), 1.0, 6.0, ((0, 16),))
    prefill_query_rows = draw_prefill_query_rows(jax.random.fold_in(jax.random.fold_in(streams_of[15], part), 71), part)
    prefill_key_values = draw_prefill_key_values(jax.random.fold_in(jax.random.fold_in(streams_of[15], part), 71), part)
    decode_query_rows = draw_decode_query_rows(jax.random.fold_in(jax.random.fold_in(streams_of[15], part), 71), part)
    decode_key_values = centred(part_keys[5], (2, DECODE_COUNT, LOCAL_KV_HEADS * HEAD_SIZE), 1.0, 6.0, ((1, 16), (2, 2)))
    cache = draw_cache(jax.random.fold_in(jax.random.fold_in(streams_of[15], part), 71), part)
    cache_len = plant(jax.random.randint(part_keys[7], (DECODE_COUNT,), 2, CACHE_POSITIONS + 1), jax.random.fold_in(part_keys[7], 1), 2, CACHE_POSITIONS).astype(jnp.int32)
    sinks = jnp.clip(-1.0 + 6.0 * jax.random.uniform(streams_of[8], (QUERY_HEADS,), jnp.float32) ** shard_levels(streams_of[8], (QUERY_HEADS,), ((0, 2),), -0.2, 0.2), -1.0, 5.0)
    o_weight = centred(streams_of[9], (QUERY_HEADS * HEAD_SIZE, D), (QUERY_HEADS * HEAD_SIZE) ** -0.5, 0.125, ((0, 2), (1, 16)))
    norm_gain = jnp.clip(1.0 + 0.1 * jax.random.normal(streams_of[10], (D,), jnp.float32), 0.5, 1.5)
    expert_ids_keys = jax.random.split(jax.random.fold_in(part_keys[11], 1), TOKENS // TOK_DEV)
    expert_ids_turns = jax.random.permutation(jax.random.fold_in(part_keys[11], 3), TOKENS // TOK_DEV)
    expert_ids = jax.vmap(lambda own, number: shared_out(jax.random.fold_in(part_keys[11], 2), own, number, TOK_DEV, EXPERTS, TOPK, SLOT, 2))(expert_ids_keys, expert_ids_turns).reshape((TOKENS, TOPK))
    route_logits = centred(part_keys[12], (TOKENS, TOPK), 1.5, 6.0, ((0, 16),), jnp.float32)
    w_gate_up = centred(streams_of[13], (2 * EXPERTS, 2, D, FF // 2), D ** -0.5, 0.15625, ((0, 16), (3, 2)))
    w_down = centred(streams_of[14], (2 * EXPERTS, FF // 2, D), FF ** -0.5, 0.15625, ((0, 16), (1, 2)))
    return {"x_pre": x_pre, "x_dec": x_dec, "prefill_query_rows": prefill_query_rows, "prefill_key_values": prefill_key_values, "decode_query_rows": decode_query_rows, "decode_key_values": decode_key_values, "cache": cache, "cache_len": cache_len, "sinks": sinks, "o_weight": o_weight, "norm_gain": norm_gain, "expert_ids": expert_ids, "route_logits": route_logits, "w_gate_up": w_gate_up, "w_down": w_down}


EPS = 1e-05

def softmax_probability(scores, sink_logit_bias):
    top = jnp.maximum(lax.optimization_barrier(jnp.max(scores, axis=-1, keepdims=True)), sink_logit_bias)
    expo = jnp.exp(scores - top)
    total = lax.optimization_barrier(jnp.sum(expo, axis=-1, keepdims=True)) + jnp.exp(sink_logit_bias - top)
    return (expo / total).astype(jnp.bfloat16)

def prefill_attention(prefill_query_rows, prefill_key_values, sinks):
    head_group = QUERY_HEADS // LOCAL_KV_HEADS
    block_list = PREFILL_TOKENS // PREFILL_LOCAL
    key_rows = prefill_key_values[0].reshape(block_list, PREFILL_LOCAL, LOCAL_KV_HEADS, HEAD_SIZE)
    value_rows = prefill_key_values[1].reshape(block_list, PREFILL_LOCAL, LOCAL_KV_HEADS, HEAD_SIZE)
    query_rows = prefill_query_rows.reshape(block_list, PREFILL_LOCAL, LOCAL_KV_HEADS, head_group, HEAD_SIZE)
    sink_logit_bias = sinks.reshape(LOCAL_KV_HEADS, head_group)[None, :, :, None]
    places = jnp.arange(PREFILL_LOCAL, dtype=jnp.int32)
    visible = places[None, :] <= places[:, None]

    def one_block(args):
        rows, block_keys, block_values = args
        scores = jnp.einsum('qhgd,khd->qhgk', rows.astype(jnp.float32), block_keys.astype(jnp.float32)) * HEAD_SIZE ** (-0.5)
        scores = jnp.where(visible[:, None, None, :], scores, -jnp.inf)
        weight_matrix = softmax_probability(scores, sink_logit_bias)
        out = jnp.einsum('qhgk,khd->qhgd', weight_matrix.astype(jnp.float32), block_values.astype(jnp.float32))
        return out.astype(jnp.bfloat16).reshape(PREFILL_LOCAL, QUERY_HEADS * HEAD_SIZE)
    return lax.map(one_block, (query_rows, key_rows, value_rows)).reshape(PREFILL_TOKENS, QUERY_HEADS * HEAD_SIZE)

def decode_attention(decode_query_rows, decode_key_values, cache, cache_len, sinks):
    head_group = QUERY_HEADS // LOCAL_KV_HEADS
    query_rows = decode_query_rows.reshape(DECODE_COUNT, LOCAL_KV_HEADS, head_group, HEAD_SIZE).astype(jnp.float32)
    cached_key_rows = cache[0].reshape(DECODE_COUNT, CACHE_POSITIONS, LOCAL_KV_HEADS, HEAD_SIZE).astype(jnp.float32)
    cached_value_rows = cache[1].reshape(DECODE_COUNT, CACHE_POSITIONS, LOCAL_KV_HEADS, HEAD_SIZE).astype(jnp.float32)
    own_key_rows = decode_key_values[0].reshape(DECODE_COUNT, LOCAL_KV_HEADS, HEAD_SIZE).astype(jnp.float32)
    own_value_rows = decode_key_values[1].reshape(DECODE_COUNT, LOCAL_KV_HEADS, HEAD_SIZE).astype(jnp.float32)
    past_positions = jnp.einsum('shgd,sjhd->shgj', query_rows, cached_key_rows) * HEAD_SIZE ** (-0.5)
    live = jnp.arange(CACHE_POSITIONS, dtype=jnp.int32)[None, :] < cache_len[:, None]
    past_positions = jnp.where(live[:, None, None, :], past_positions, -jnp.inf)
    own_token = jnp.einsum('shgd,shd->shg', query_rows, own_key_rows)[..., None] * HEAD_SIZE ** (-0.5)
    weight_matrix = softmax_probability(jnp.concatenate([past_positions, own_token], axis=-1), sinks.reshape(LOCAL_KV_HEADS, head_group)[None, :, :, None])
    weight_matrix = weight_matrix.astype(jnp.float32)
    out = jnp.einsum('shgj,sjhd->shgd', weight_matrix[..., :CACHE_POSITIONS], cached_value_rows)
    out = out + weight_matrix[..., CACHE_POSITIONS:] * own_value_rows[:, :, None, :]
    return out.astype(jnp.bfloat16).reshape(DECODE_COUNT, QUERY_HEADS * HEAD_SIZE)

def device_major(pre, dec):
    first = pre.reshape(N_EP, PREFILL_LOCAL, pre.shape[-1])
    second = dec.reshape(N_EP, DEC_DEV, dec.shape[-1])
    return jnp.concatenate([first, second], axis=1).reshape(N_EP * (PREFILL_LOCAL + DEC_DEV), pre.shape[-1])

def reference(x_pre, x_dec, prefill_query_rows, prefill_key_values, decode_query_rows, decode_key_values, cache, cache_len, sinks, o_weight, norm_gain, expert_ids, route_logits, w_gate_up, w_down):
    attended = device_major(prefill_attention(prefill_query_rows, prefill_key_values, sinks), decode_attention(decode_query_rows, decode_key_values, cache, cache_len, sinks))
    stream = device_major(x_pre, x_dec).astype(jnp.float32) + jnp.dot(attended, o_weight, preferred_element_type=jnp.float32)
    mean_sq = lax.optimization_barrier(jnp.mean(stream * stream, axis=-1, keepdims=True))
    normed = (stream * lax.rsqrt(mean_sq + EPS) * norm_gain).astype(jnp.bfloat16)
    flat_ids = expert_ids.reshape(-1)
    capacity = N_EP * SLOT
    quarter = FF // 4

    def one_holder(outputs, args):
        expert, gate_up, down = args
        chosen = flat_ids == expert
        picked = jnp.nonzero(chosen, size=capacity, fill_value=0)[0].astype(jnp.int32)
        count = jnp.sum(chosen.astype(jnp.int32))
        live = (jnp.arange(capacity, dtype=jnp.int32) < count).astype(jnp.float32)
        rows = normed[picked // TOPK]
        gate = jnp.dot(rows, gate_up[0], preferred_element_type=jnp.float32)
        upper = jnp.dot(rows, gate_up[1], preferred_element_type=jnp.float32)
        hidden = ((upper + 1.0) * gate * jax.nn.sigmoid(1.702 * gate)).astype(jnp.bfloat16)
        lower_part = jnp.dot(hidden[:, :quarter], down[:quarter], preferred_element_type=jnp.float32).astype(jnp.bfloat16)
        upper_part = jnp.dot(hidden[:, quarter:], down[quarter:], preferred_element_type=jnp.float32).astype(jnp.bfloat16)
        lower_part, upper_part = lax.optimization_barrier((lower_part, upper_part))
        result = (lower_part.astype(jnp.float32) + upper_part.astype(jnp.float32)).astype(jnp.bfloat16)
        result = lax.optimization_barrier(result).astype(jnp.float32) * live[:, None]
        return (outputs.at[picked].add(result), None)
    holders = jnp.arange(2 * EXPERTS, dtype=jnp.int32) // 2
    outputs, _ = lax.scan(one_holder, jnp.zeros((TOKENS * TOPK, D), jnp.float32), (holders, w_gate_up, w_down))
    mix = jax.nn.softmax(route_logits, axis=-1)
    moe = lax.optimization_barrier(jnp.sum(outputs.reshape(TOKENS, TOPK, D) * mix[:, :, None], axis=1))
    return (stream + moe).astype(jnp.bfloat16)
```

```python
import functools

import jax
import jax.numpy as jnp
from jax import lax
from jax.experimental import pallas as pl
from jax.experimental.pallas import tpu as pltpu
from jax.sharding import PartitionSpec as P

HEAD_SIZE = 64


EPS = 1e-05


def softmax_probability(scores, sink_logit_bias):
    top = jnp.maximum(jnp.max(scores, axis=-1, keepdims=True), sink_logit_bias)
    expo = jnp.exp(scores - top)
    total = jnp.sum(expo, axis=-1, keepdims=True) + jnp.exp(sink_logit_bias - top)
    return (expo / total).astype(jnp.bfloat16)


def rms_norm(stream, gain):
    mean_sq = jnp.mean(stream * stream, axis=-1, keepdims=True)
    return (stream * lax.rsqrt(mean_sq + EPS) * gain).astype(jnp.bfloat16)


def attention_rows(
    x_pre,
    x_dec,
    prefill_query_rows,
    prefill_key_values,
    decode_query_rows,
    decode_key_values,
    cache,
    cache_len,
    sinks):
    pre_rows, width = x_pre.shape
    dec_rows = x_dec.shape[0]
    kv_heads = prefill_key_values.shape[2] // HEAD_SIZE
    q_heads = sinks.shape[0]
    head_group = q_heads // kv_heads
    kv_max = cache.shape[2]
    scale = HEAD_SIZE ** (-0.5)
    sink_logit_bias = sinks.reshape(kv_heads, head_group)[None, :, :, None]
    keys_here = prefill_key_values[0].reshape(pre_rows, kv_heads, HEAD_SIZE)
    values_here = prefill_key_values[1].reshape(pre_rows, kv_heads, HEAD_SIZE)
    query_rows = prefill_query_rows.reshape(pre_rows, kv_heads, head_group, HEAD_SIZE)
    scores = (
        jnp.einsum("qhgd,khd->qhgk", query_rows, keys_here, preferred_element_type=jnp.float32)
        * scale
    )
    places = jnp.arange(pre_rows, dtype=jnp.int32)
    visible = places[None, :] <= places[:, None]
    scores = jnp.where(visible[:, None, None, :], scores, -jnp.inf)
    weight_matrix = softmax_probability(scores, sink_logit_bias)
    pre_out = jnp.einsum(
        "qhgk,khd->qhgd", weight_matrix, values_here, preferred_element_type=jnp.float32
    )
    pre_out = pre_out.astype(jnp.bfloat16).reshape(pre_rows, q_heads * HEAD_SIZE)
    dec_queries = decode_query_rows.reshape(dec_rows, kv_heads, head_group, HEAD_SIZE)
    cached_key_rows = cache[0].reshape(dec_rows, kv_max, kv_heads, HEAD_SIZE)
    cached_value_rows = cache[1].reshape(dec_rows, kv_max, kv_heads, HEAD_SIZE)
    own_key_rows = decode_key_values[0].reshape(dec_rows, kv_heads, HEAD_SIZE)
    own_value_rows = decode_key_values[1].reshape(dec_rows, kv_heads, HEAD_SIZE)
    past_positions = (
        jnp.einsum(
            "shgd,sjhd->shgj", dec_queries, cached_key_rows, preferred_element_type=jnp.float32
        )
        * scale
    )
    live = jnp.arange(kv_max, dtype=jnp.int32)[None, :] < cache_len[:, None]
    past_positions = jnp.where(live[:, None, None, :], past_positions, -jnp.inf)
    own_token = (
        jnp.einsum("shgd,shd->shg", dec_queries, own_key_rows, preferred_element_type=jnp.float32)[
            ..., None
        ]
        * scale
    )
    dec_weights = softmax_probability(
        jnp.concatenate([past_positions, own_token], axis=-1), sink_logit_bias
    )
    dec_out = jnp.einsum(
        "shgj,sjhd->shgd",
        dec_weights[..., :kv_max],
        cached_value_rows,
        preferred_element_type=jnp.float32,
    )
    dec_out = (
        dec_out
        + dec_weights[..., kv_max:].astype(jnp.float32)
        * own_value_rows.astype(jnp.float32)[:, :, None, :]
    )
    dec_out = dec_out.astype(jnp.bfloat16).reshape(dec_rows, q_heads * HEAD_SIZE)
    attn_rows = jnp.concatenate([pre_out, dec_out], axis=0)
    return attn_rows
def general_path(
    x_pre,
    x_dec,
    prefill_query_rows,
    prefill_key_values,
    decode_query_rows,
    decode_key_values,
    cache,
    cache_len,
    sinks,
    o_weight,
    norm_gain,
    expert_ids,
    route_logits,
    w_gate_up,
    w_down,
):
    attn_rows = attention_rows(
        x_pre,
        x_dec,
        prefill_query_rows,
        prefill_key_values,
        decode_query_rows,
        decode_key_values,
        cache,
        cache_len,
        sinks,
    )
    width = x_pre.shape[1]
    resid = jnp.concatenate([x_pre, x_dec], axis=0).astype(jnp.float32)
    half = attn_rows.shape[0] // 2
    mine = lax.axis_index("hp") * half
    head_part = jnp.dot(
        attn_rows,
        lax.all_gather(o_weight, "ep", axis=1, tiled=True),
        preferred_element_type=jnp.float32,
    )
    summed = lax.psum_scatter(head_part, "hp", scatter_dimension=0, tiled=True)
    stream = lax.dynamic_slice_in_dim(resid, mine, half, 0) + summed
    normed = lax.all_gather(rms_norm(stream, norm_gain), "hp", axis=0, tiled=True)
    tokens_here, topk = expert_ids.shape
    holders = lax.axis_size("ep")
    experts = holders // 2
    slot = min(
        tokens_here, 2 * ((3 * max(1, (tokens_here * topk + experts - 1) // experts) + 3) // 4)
    )
    plane = slot // 2
    flat_ids = expert_ids.reshape(-1)
    onehot = (flat_ids[:, None] == jnp.arange(experts, dtype=jnp.int32)[None, :]).astype(jnp.int32)
    rank = jnp.sum(jnp.cumsum(onehot, axis=0) * onehot, axis=1) - 1
    position = (flat_ids * slot + rank).reshape(tokens_here, topk)
    columns = jnp.arange(experts * slot, dtype=jnp.int32)[None, None, :] == position[:, :, None]
    picked_rows = jnp.any(columns, axis=1).T.astype(jnp.bfloat16)
    per_expert = (
        jnp.dot(picked_rows, normed, preferred_element_type=jnp.float32)
        .astype(jnp.bfloat16)
        .reshape(experts, slot, width)
    )
    send = jnp.repeat(per_expert, 2, axis=0)
    own_plane = lax.dynamic_slice_in_dim(send, lax.axis_index("hp") * plane, plane, 1)
    arrived_plane = lax.all_to_all(own_plane, "ep", split_axis=0, concat_axis=0, tiled=True)
    arrived = lax.all_gather(arrived_plane, "hp", axis=1, tiled=True)
    rows = arrived.reshape(-1, width)
    gate = jnp.dot(rows, w_gate_up[0, 0], preferred_element_type=jnp.float32)
    upper = jnp.dot(rows, w_gate_up[0, 1], preferred_element_type=jnp.float32)
    hidden = ((upper + 1.0) * gate * jax.nn.sigmoid(1.702 * gate)).astype(jnp.bfloat16)
    partial_out = jnp.dot(hidden, w_down[0], preferred_element_type=jnp.float32).reshape(
        -1, slot, width
    )
    share = lax.psum_scatter(
        partial_out.astype(jnp.bfloat16), "hp", scatter_dimension=1, tiled=True
    )
    returned = lax.all_to_all(share, "ep", split_axis=0, concat_axis=0, tiled=True)
    mix = jax.nn.softmax(route_logits, axis=-1)
    blend = jnp.sum(jnp.where(columns, mix[:, :, None], 0.0), axis=1).reshape(
        tokens_here, experts, slot
    )
    blend = jnp.repeat(blend, 2, axis=1)
    blend_plane = lax.dynamic_slice_in_dim(blend, lax.axis_index("hp") * plane, plane, 2).reshape(
        tokens_here, holders * plane
    )
    terms = jnp.dot(
        blend_plane,
        returned.reshape(-1, width).astype(jnp.float32),
        precision=lax.Precision.HIGHEST,
    )
    moe = lax.psum_scatter(
        terms.astype(jnp.bfloat16), "hp", scatter_dimension=0, tiled=True
    ).astype(jnp.float32)
    return (stream + moe).astype(jnp.bfloat16)


MESH = pl.DeviceIdType.MESH
SIDE = 2


def layer_kernel(
    depth_z,
    attn_ref,
    wo_ref,
    x_ref,
    gain_ref,
    blend_ref,
    gu_hbm,
    dn_hbm,
    out_ref,
    wo_all,
    mix_all,
    mix_cols,
    proj,
    proj_in,
    tok,
    part_out,
    from_core,
    from_first,
    mid,
    from_z,
    last_out,
    from_last,
    gu,
    dn,
    send_sem,
    recv_sem,
    load_sem,
):
    zs = depth_z
    me = lax.axis_index("ep")
    core = lax.axis_index("hp")
    x, y, z = lax.rem(me, 2), lax.rem(me // 2, 2), me // 4
    other = 1 - core
    to_x = {"ep": z * 4 + y * 2 + (1 - x)}
    to_y = {"ep": z * 4 + (1 - y) * 2 + x}
    to_z = [None] + [{"ep": lax.rem(z + d, zs) * 4 + y * 2 + x} for d in range(1, zs)]
    to_core = {"hp": other}

    load_gu = pltpu.make_async_copy(gu_hbm, gu, load_sem.at[0])
    load_dn = pltpu.make_async_copy(dn_hbm, dn, load_sem.at[1])
    load_gu.start()
    load_dn.start()

    barrier = pltpu.get_barrier_semaphore()
    partners = [to_x, to_y, to_core] + to_z[1:]
    for partner in partners:
        pl.semaphore_signal(barrier, inc=1, device_id=partner, device_id_type=MESH)
    for p in range(2):
        wo_all[p, z, y, x] = wo_ref[p]
    mix_all[z, y, x] = blend_ref[...]
    pl.semaphore_wait(barrier, len(partners))

    sent = []

    def push(source, target, device):
        i = len(sent)
        copy = pltpu.make_async_remote_copy(
            src_ref=source,
            dst_ref=target,
            send_sem=send_sem.at[i],
            recv_sem=recv_sem.at[i],
            device_id=device,
            device_id_type=MESH,
        )
        copy.start()
        sent.append(copy)
        return copy

    def gather(lanes):
        def near(first_y, zz, flip):
            return (zz, 1 - y if flip else y, x) if first_y else (zz, y, 1 - x if flip else x)

        first, second, across = [], [], []
        for view, first_y in lanes:
            own = view(z, y, x)
            first.append(push(own, own, to_y if first_y else to_x))
        for view, first_y in lanes:
            own = view(z, y, x)
            second.append([[push(own, own, to_z[d]) for d in range(1, zs)]])
        for view, first_y in lanes:
            own = view(z, y, x)
            across.append([push(own, own, to_x if first_y else to_y)])
        for n, (view, first_y) in enumerate(lanes):
            first[n].wait_recv()
            block = view(*near(first_y, z, True))
            second[n].append([push(block, block, to_z[d]) for d in range(1, zs)])
            across[n].append(push(block, block, to_x if first_y else to_y))
        for flip in (False, True):
            for d in range(1, zs):
                for n, (view, first_y) in enumerate(lanes):
                    second[n][int(flip)][d - 1].wait_recv()
                    block = view(*near(first_y, lax.rem(z - d + zs, zs), flip))
                    across[n].append(push(block, block, to_x if first_y else to_y))
        return across

    def settle(across):
        for copies in across:
            for copy in copies:
                copy.wait_recv()

    settle(
        gather(
            [
                (lambda *at: wo_all.at[(0, *at)], True),
                (lambda *at: wo_all.at[(1, *at)], False),
                (lambda *at: mix_all.at[at], True),
            ]
        )
    )

    rows, inner = attn_ref.shape
    half = rows // 2
    split = inner // 2
    width = x_ref.shape[1]
    nt = (((1,), (1,)), ((), ()))
    piece = width // zs
    for j in range(zs):
        total = 0.0
        for p in range(2):
            weight = wo_all[p, j].reshape(piece, split)
            total = total + lax.dot_general(
                attn_ref[:, p * split : (p + 1) * split],
                weight,
                nt,
                preferred_element_type=jnp.float32,
            )
        proj[0, :, j * piece : (j + 1) * piece] = total[:half]
        proj[1, :, j * piece : (j + 1) * piece] = total[half:]
    exchange = push(proj.at[other], proj_in, to_core)

    expert = me // 2
    experts_rows = jnp.concatenate(
        [
            mix_all[a, b, c, pl.ds(expert, 1), :]
            for a in range(zs)
            for b in range(2)
            for c in range(2)
        ],
        axis=0,
    )
    mix_cols[...] = experts_rows.T

    exchange.wait_recv()
    mine = pl.ds(pl.multiple_of(core * half, half), half)
    stream = x_ref[mine, :].astype(jnp.float32) + (proj[core] + proj_in[...])
    proj[core] = stream
    mean_sq = jnp.mean(stream * stream, axis=-1, keepdims=True)
    normed = (stream * lax.rsqrt(mean_sq + EPS) * gain_ref[...]).astype(jnp.bfloat16)
    r = half // 2
    for p in range(2):
        tok[core, p, z, y, x] = normed[p * r : (p + 1) * r]
    across = gather(
        [
            (lambda *at: tok.at[(core, 0, *at)], True),
            (lambda *at: tok.at[(core, 1, *at)], False),
        ]
    )
    whole = lambda p: tok.at[core, p]
    near0 = tok.at[core, 0, :, :, x]
    near1 = tok.at[core, 1, :, y]
    over = [[push(near0, near0, to_core)], [push(near1, near1, to_core)]]
    far0 = tok.at[core, 0, :, :, 1 - x]
    far1 = tok.at[core, 1, :, 1 - y]
    settle(across[:1])
    over[0].append(push(far0, far0, to_core))
    settle(across[1:])
    over[1].append(push(far1, far1, to_core))
    load_gu.wait()
    load_dn.wait()

    blocks = zs * 4

    def expert_rows(side, p):
        rows_in = tok[side, p].reshape(blocks * r, width)
        gate = jnp.dot(rows_in, gu[0], preferred_element_type=jnp.float32)
        upper = jnp.dot(rows_in, gu[1], preferred_element_type=jnp.float32)
        cols = mix_cols[pl.ds(pl.multiple_of(side * half + p * r, r), r), :]
        scale = jnp.concatenate([cols[:, b : b + 1] for b in range(blocks)], axis=0)
        hidden = (upper + 1.0) * gate * jax.nn.sigmoid(1.702 * gate) * scale
        result = jnp.dot(hidden.astype(jnp.bfloat16), dn[...], preferred_element_type=jnp.float32)
        return result.reshape(zs, 2, 2, r, width)

    back = []
    for p in range(2):
        for copy in over[p]:
            copy.wait_recv()
        part_out[other, p] = expert_rows(other, p).astype(jnp.bfloat16)
        back.append(push(part_out.at[other, p], from_core.at[p], to_core))

    firsts = []
    for p in range(2):
        result = expert_rows(core, p)
        back[p].wait_recv()
        part_out[core, p] = (result + from_core[p].astype(jnp.float32)).astype(jnp.bfloat16)
        copies = []
        for d in list(range(1, zs)) + [0]:
            zt = lax.rem(z + d, zs)
            if p == 0:
                source, device = part_out.at[core, 0, zt, :, 1 - x], to_x
            else:
                source, device = part_out.at[core, 1, zt, 1 - y], to_y
            copies.append(push(source, from_first.at[p, d], device))
        firsts.append(copies)
    order = list(range(1, zs)) + [0]
    seconds = [[], []]
    for k, d in enumerate(order):
        for p in range(2):
            zt = lax.rem(z + d, zs)
            firsts[p][k].wait_recv()
            kept = part_out[core, 0, zt, :, x] if p == 0 else part_out[core, 1, zt, y]
            total = kept.astype(jnp.float32) + from_first[p, d].astype(jnp.float32)
            mid[p, d] = total.astype(jnp.bfloat16)
            if d:
                seconds[p].append(push(mid.at[p, d], from_z.at[p, d - 1], to_z[d]))
    lasts = []
    for p in range(2):
        total = mid[p, 0].astype(jnp.float32)
        for d in range(1, zs):
            seconds[p][d - 1].wait_recv()
            total = total + from_z[p, d - 1].astype(jnp.float32)
        last_out[p] = total
        from_last[p, 0] = last_out[p, 1 - (y if p == 0 else x)].astype(jnp.bfloat16)
        lasts.append(push(from_last.at[p, 0], from_last.at[p, 1], to_y if p == 0 else to_x))
    for p in range(2):
        lasts[p].wait_recv()
        total = last_out[p, y if p == 0 else x] + from_last[p, 1].astype(jnp.float32)
        out_ref[p * r : (p + 1) * r, :] = (proj[core, p * r : (p + 1) * r, :] + total).astype(
            jnp.bfloat16
        )
    for copy in sent:
        copy.wait_send()


def fused_path(
    holders,
    x_pre,
    x_dec,
    prefill_query_rows,
    prefill_key_values,
    decode_query_rows,
    decode_key_values,
    cache,
    cache_len,
    sinks,
    o_weight,
    norm_gain,
    expert_ids,
    route_logits,
    w_gate_up,
    w_down,
):
    attn_rows = attention_rows(
        x_pre,
        x_dec,
        prefill_query_rows,
        prefill_key_values,
        decode_query_rows,
        decode_key_values,
        cache,
        cache_len,
        sinks,
    )
    tokens, inner = attn_rows.shape
    width = x_pre.shape[1]
    hidden = w_down.shape[1]
    columns = o_weight.shape[1]
    zs = holders // 4
    half, r = tokens // 2, tokens // 4
    experts = holders // 2
    resid = jnp.concatenate([x_pre, x_dec], axis=0)
    wo = o_weight.reshape(2, inner // 2, columns).transpose(0, 2, 1)
    mix = jax.nn.softmax(route_logits, axis=-1)
    chosen = expert_ids[None, :, :] == jnp.arange(experts, dtype=jnp.int32)[:, None, None]
    blend = jnp.sum(jnp.where(chosen, mix[None], 0.0), axis=-1)
    blend = jnp.pad(blend, ((0, 0), (0, -tokens % 128)))
    bf = jnp.bfloat16
    grid = (zs, 2, 2)
    return pl.pallas_call(
        functools.partial(layer_kernel, zs),
        out_shape=jax.ShapeDtypeStruct((half, width), bf),
        in_specs=[pl.BlockSpec(memory_space=pltpu.VMEM)] * 5
        + [pl.BlockSpec(memory_space=pl.ANY)] * 2,
        out_specs=pl.BlockSpec(memory_space=pltpu.VMEM),
        scratch_shapes=[
            pltpu.VMEM((2, *grid, columns, inner // 2), bf),
            pltpu.VMEM((*grid, *blend.shape), jnp.float32),
            pltpu.VMEM((blend.shape[1], holders), jnp.float32),
            pltpu.VMEM((2, half, width), jnp.float32),
            pltpu.VMEM((half, width), jnp.float32),
            pltpu.VMEM((2, 2, *grid, r, width), bf),
            pltpu.VMEM((2, 2, *grid, r, width), bf),
            pltpu.VMEM((2, *grid, r, width), bf),
            pltpu.VMEM((2, zs, 2, r, width), bf),
            pltpu.VMEM((2, zs, 2, r, width), bf),
            pltpu.VMEM((2, zs - 1, 2, r, width), bf),
            pltpu.VMEM((2, 2, r, width), jnp.float32),
            pltpu.VMEM((2, 2, r, width), bf),
            pltpu.VMEM((2, width, hidden), bf),
            pltpu.VMEM((hidden, width), bf),
            pltpu.SemaphoreType.DMA((192,)),
            pltpu.SemaphoreType.DMA((192,)),
            pltpu.SemaphoreType.DMA((2,)),
        ],
        compiler_params=pltpu.CompilerParams(
            collective_id=0, has_side_effects=True, vmem_limit_bytes=60 * 2**20
        ),
    )(attn_rows, wo, resid, norm_gain.reshape(1, width), blend, w_gate_up[0], w_down[0])


def on_device(holders, *args):
    x_pre, x_dec, o_weight = args[0], args[1], args[9]
    tokens = x_pre.shape[0] + x_dec.shape[0]
    gathered = 2 * holders * (tokens * x_pre.shape[1] * 4 + o_weight.size)
    if holders % 4 == 0 and holders >= 8 and tokens % 64 == 0 and gathered < 32 * 2**20:
        return fused_path(holders, *args)
    return general_path(*args)


def solution(mesh):
    placed = (
        P(("groups", "ep"), None),
        P(("groups", "ep"), None),
        P(("groups", "ep"), "hp"),
        P(None, ("groups", "ep"), "hp"),
        P(("groups", "ep"), "hp"),
        P(None, ("groups", "ep"), "hp"),
        P(None, ("groups", "ep"), None, "hp"),
        P(("groups", "ep")),
        P("hp"),
        P("hp", "ep"),
        P(),
        P(("groups", "ep"), None),
        P(("groups", "ep"), None),
        P("ep", None, None, "hp"),
        P("ep", "hp", None),
    )
    return jax.shard_map(
        functools.partial(on_device, mesh.shape["ep"]),
        mesh=mesh,
        in_specs=placed,
        out_specs=P(("groups", "ep", "hp"), None),
        check_vma=False,
    )
```

```python
import functools

import jax
import jax.numpy as jnp
from jax import lax
from jax.experimental import pallas as pl
from jax.experimental.pallas import tpu as pltpu
from jax.sharding import PartitionSpec as P

HEAD_SIZE = 64


EPS = 1e-05


def softmax_probability(scores, sink_logit_bias):
    top = jnp.maximum(jnp.max(scores, axis=-1, keepdims=True), sink_logit_bias)
    expo = jnp.exp(scores - top)
    total = jnp.sum(expo, axis=-1, keepdims=True) + jnp.exp(sink_logit_bias - top)
    return (expo / total).astype(jnp.bfloat16)


def rms_norm(stream, gain):
    mean_sq = jnp.mean(stream * stream, axis=-1, keepdims=True)
    return (stream * lax.rsqrt(mean_sq + EPS) * gain).astype(jnp.bfloat16)


def attention_rows(
    x_pre,
    x_dec,
    prefill_query_rows,
    prefill_key_values,
    decode_query_rows,
    decode_key_values,
    cache,
    cache_len,
    sinks):
    pre_rows, width = x_pre.shape
    dec_rows = x_dec.shape[0]
    kv_heads = prefill_key_values.shape[2] // HEAD_SIZE
    q_heads = sinks.shape[0]
    head_group = q_heads // kv_heads
    kv_max = cache.shape[2]
    scale = HEAD_SIZE ** (-0.5)
    sink_logit_bias = sinks.reshape(kv_heads, head_group)[None, :, :, None]
    keys_here = prefill_key_values[0].reshape(pre_rows, kv_heads, HEAD_SIZE)
    values_here = prefill_key_values[1].reshape(pre_rows, kv_heads, HEAD_SIZE)
    query_rows = prefill_query_rows.reshape(pre_rows, kv_heads, head_group, HEAD_SIZE)
    scores = (
        jnp.einsum("qhgd,khd->qhgk", query_rows, keys_here, preferred_element_type=jnp.float32)
        * scale
    )
    places = jnp.arange(pre_rows, dtype=jnp.int32)
    visible = places[None, :] <= places[:, None]
    scores = jnp.where(visible[:, None, None, :], scores, -jnp.inf)
    weight_matrix = softmax_probability(scores, sink_logit_bias)
    pre_out = jnp.einsum(
        "qhgk,khd->qhgd", weight_matrix, values_here, preferred_element_type=jnp.float32
    )
    pre_out = pre_out.astype(jnp.bfloat16).reshape(pre_rows, q_heads * HEAD_SIZE)
    dec_queries = decode_query_rows.reshape(dec_rows, kv_heads, head_group, HEAD_SIZE)
    cached_key_rows = cache[0].reshape(dec_rows, kv_max, kv_heads, HEAD_SIZE)
    cached_value_rows = cache[1].reshape(dec_rows, kv_max, kv_heads, HEAD_SIZE)
    own_key_rows = decode_key_values[0].reshape(dec_rows, kv_heads, HEAD_SIZE)
    own_value_rows = decode_key_values[1].reshape(dec_rows, kv_heads, HEAD_SIZE)
    past_positions = (
        jnp.einsum(
            "shgd,sjhd->shgj", dec_queries, cached_key_rows, preferred_element_type=jnp.float32
        )
        * scale
    )
    live = jnp.arange(kv_max, dtype=jnp.int32)[None, :] < cache_len[:, None]
    past_positions = jnp.where(live[:, None, None, :], past_positions, -jnp.inf)
    own_token = (
        jnp.einsum("shgd,shd->shg", dec_queries, own_key_rows, preferred_element_type=jnp.float32)[
            ..., None
        ]
        * scale
    )
    dec_weights = softmax_probability(
        jnp.concatenate([past_positions, own_token], axis=-1), sink_logit_bias
    )
    dec_out = jnp.einsum(
        "shgj,sjhd->shgd",
        dec_weights[..., :kv_max],
        cached_value_rows,
        preferred_element_type=jnp.float32,
    )
    dec_out = (
        dec_out
        + dec_weights[..., kv_max:].astype(jnp.float32)
        * own_value_rows.astype(jnp.float32)[:, :, None, :]
    )
    dec_out = dec_out.astype(jnp.bfloat16).reshape(dec_rows, q_heads * HEAD_SIZE)
    attn_rows = jnp.concatenate([pre_out, dec_out], axis=0)
    return attn_rows
def general_path(
    x_pre,
    x_dec,
    prefill_query_rows,
    prefill_key_values,
    decode_query_rows,
    decode_key_values,
    cache,
    cache_len,
    sinks,
    o_weight,
    norm_gain,
    expert_ids,
    route_logits,
    w_gate_up,
    w_down,
):
    attn_rows = attention_rows(
        x_pre,
        x_dec,
        prefill_query_rows,
        prefill_key_values,
        decode_query_rows,
        decode_key_values,
        cache,
        cache_len,
        sinks,
    )
    width = x_pre.shape[1]
    resid = jnp.concatenate([x_pre, x_dec], axis=0).astype(jnp.float32)
    half = attn_rows.shape[0] // 2
    mine = lax.axis_index("hp") * half
    head_part = jnp.dot(
        attn_rows,
        lax.all_gather(o_weight, "ep", axis=1, tiled=True),
        preferred_element_type=jnp.float32,
    )
    summed = lax.psum_scatter(head_part, "hp", scatter_dimension=0, tiled=True)
    stream = lax.dynamic_slice_in_dim(resid, mine, half, 0) + summed
    normed = lax.all_gather(rms_norm(stream, norm_gain), "hp", axis=0, tiled=True)
    tokens_here, topk = expert_ids.shape
    holders = lax.axis_size("ep")
    experts = holders // 2
    slot = min(
        tokens_here, 2 * ((3 * max(1, (tokens_here * topk + experts - 1) // experts) + 3) // 4)
    )
    plane = slot // 2
    flat_ids = expert_ids.reshape(-1)
    onehot = (flat_ids[:, None] == jnp.arange(experts, dtype=jnp.int32)[None, :]).astype(jnp.int32)
    rank = jnp.sum(jnp.cumsum(onehot, axis=0) * onehot, axis=1) - 1
    position = (flat_ids * slot + rank).reshape(tokens_here, topk)
    columns = jnp.arange(experts * slot, dtype=jnp.int32)[None, None, :] == position[:, :, None]
    picked_rows = jnp.any(columns, axis=1).T.astype(jnp.bfloat16)
    per_expert = (
        jnp.dot(picked_rows, normed, preferred_element_type=jnp.float32)
        .astype(jnp.bfloat16)
        .reshape(experts, slot, width)
    )
    send = jnp.repeat(per_expert, 2, axis=0)
    own_plane = lax.dynamic_slice_in_dim(send, lax.axis_index("hp") * plane, plane, 1)
    arrived_plane = lax.all_to_all(own_plane, "ep", split_axis=0, concat_axis=0, tiled=True)
    arrived = lax.all_gather(arrived_plane, "hp", axis=1, tiled=True)
    rows = arrived.reshape(-1, width)
    gate = jnp.dot(rows, w_gate_up[0, 0], preferred_element_type=jnp.float32)
    upper = jnp.dot(rows, w_gate_up[0, 1], preferred_element_type=jnp.float32)
    hidden = ((upper + 1.0) * gate * jax.nn.sigmoid(1.702 * gate)).astype(jnp.bfloat16)
    partial_out = jnp.dot(hidden, w_down[0], preferred_element_type=jnp.float32).reshape(
        -1, slot, width
    )
    share = lax.psum_scatter(
        partial_out.astype(jnp.bfloat16), "hp", scatter_dimension=1, tiled=True
    )
    returned = lax.all_to_all(share, "ep", split_axis=0, concat_axis=0, tiled=True)
    mix = jax.nn.softmax(route_logits, axis=-1)
    blend = jnp.sum(jnp.where(columns, mix[:, :, None], 0.0), axis=1).reshape(
        tokens_here, experts, slot
    )
    blend = jnp.repeat(blend, 2, axis=1)
    blend_plane = lax.dynamic_slice_in_dim(blend, lax.axis_index("hp") * plane, plane, 2).reshape(
        tokens_here, holders * plane
    )
    terms = jnp.dot(
        blend_plane,
        returned.reshape(-1, width).astype(jnp.float32),
        precision=lax.Precision.HIGHEST,
    )
    moe = lax.psum_scatter(
        terms.astype(jnp.bfloat16), "hp", scatter_dimension=0, tiled=True
    ).astype(jnp.float32)
    return (stream + moe).astype(jnp.bfloat16)


MESH = pl.DeviceIdType.MESH
SIDE = 2


def layer_kernel(
    depth_z,
    attn_ref,
    wo_ref,
    x_ref,
    gain_ref,
    blend_ref,
    gu_hbm,
    dn_hbm,
    out_ref,
    wo_all,
    mix_all,
    mix_cols,
    attn_all,
    proj,
    proj_in,
    columns,
    kept_rows,
    tok,
    part_out,
    from_core,
    from_first,
    mid,
    from_second,
    to_send,
    from_z,
    gu,
    dn,
    send_sem,
    recv_sem,
    load_sem,
):
    zs = depth_z
    me = lax.axis_index("ep")
    core = lax.axis_index("hp")
    x, y, z = lax.rem(me, 2), lax.rem(me // 2, 2), me // 4
    other = 1 - core
    to_x = {"ep": z * 4 + y * 2 + (1 - x)}
    to_y = {"ep": z * 4 + (1 - y) * 2 + x}
    to_z = [None] + [{"ep": lax.rem(z + d, zs) * 4 + y * 2 + x} for d in range(1, zs)]
    to_core = {"hp": other}

    load_gu = pltpu.make_async_copy(gu_hbm, gu, load_sem.at[0])
    load_dn = pltpu.make_async_copy(dn_hbm, dn, load_sem.at[1])
    load_gu.start()
    load_dn.start()

    barrier = pltpu.get_barrier_semaphore()
    partners = [to_x, to_y, to_core] + to_z[1:]
    for partner in partners:
        pl.semaphore_signal(barrier, inc=1, device_id=partner, device_id_type=MESH)
    for p in range(2):
        wo_all[p, y, x] = wo_ref[p]
    mix_all[z, y, x] = blend_ref[...]
    pl.semaphore_wait(barrier, len(partners))

    sent = []

    def push(source, target, device):
        i = len(sent)
        copy = pltpu.make_async_remote_copy(
            src_ref=source,
            dst_ref=target,
            send_sem=send_sem.at[i],
            recv_sem=recv_sem.at[i],
            device_id=device,
            device_id_type=MESH,
        )
        copy.start()
        sent.append(copy)
        return copy

    def gather(lanes):
        along, second, last = [], [], []
        for view, x_next in lanes:
            own = view(z, y, x)
            along.append([push(own, own, to_z[d]) for d in range(1, zs)])
            second.append([push(own, own, to_x if x_next else to_y)])
            last.append([push(own, own, to_y if x_next else to_x)])
        for d in range(zs):
            zt = lax.rem(z - d + zs, zs)
            for n, (view, x_next) in enumerate(lanes):
                if d:
                    along[n][d - 1].wait_recv()
                    block = view(zt, y, x)
                    second[n].append(push(block, block, to_x if x_next else to_y))
                    last[n].append(push(block, block, to_y if x_next else to_x))
        for d in range(zs):
            zt = lax.rem(z - d + zs, zs)
            for n, (view, x_next) in enumerate(lanes):
                second[n][d].wait_recv()
                block = view(zt, y, 1 - x) if x_next else view(zt, 1 - y, x)
                last[n].append(push(block, block, to_y if x_next else to_x))
        return last

    def settle(across):
        for copies in across:
            for copy in copies:
                copy.wait_recv()

    rows, inner = attn_ref.shape
    half = rows // 2
    split = inner // 2
    width = x_ref.shape[1]
    piece = width // zs
    nt = (((1,), (1,)), ((), ()))

    heads = [push(attn_ref, attn_all.at[d - 1], to_z[d]) for d in range(1, zs)]
    own0, own1 = wo_all.at[0, y, x], wo_all.at[1, y, x]
    weights = [push(own0, own0, to_y), push(own1, own1, to_x)]
    weights += [push(own0, own0, to_x), push(own1, own1, to_y)]
    own = mix_all.at[z, y, x]
    mixes = [push(own, own, to_z[d]) for d in range(1, zs)]
    weights[0].wait_recv()
    near = wo_all.at[0, 1 - y, x]
    weights.append(push(near, near, to_x))
    weights[1].wait_recv()
    near = wo_all.at[1, y, 1 - x]
    weights.append(push(near, near, to_y))
    for copy in mixes:
        copy.wait_recv()
    near = mix_all.at[:, y, x]
    copy = push(near, near, to_y)
    copy.wait_recv()
    near = mix_all.at[:, :, x]
    mixes = push(near, near, to_x)
    for copy in weights[2:]:
        copy.wait_recv()
    exchange = []
    for d in range(zs):
        if d:
            heads[d - 1].wait_recv()
        queries = attn_all[d - 1] if d else attn_ref[...]
        total = 0.0
        for p in range(2):
            total = total + lax.dot_general(
                queries[:, p * split : (p + 1) * split],
                wo_all[p].reshape(piece, split),
                nt,
                preferred_element_type=jnp.float32,
            )
        proj[d, 0] = total[:half]
        proj[d, 1] = total[half:]
        exchange.append(push(proj.at[d, other], proj_in.at[d], to_core))
    returns = []
    for d in list(range(1, zs)) + [0]:
        exchange[d].wait_recv()
        if d:
            proj[d, core] = proj[d, core] + proj_in[d]
            returns.append(push(proj.at[d, core], columns.at[z], to_z[zs - d]))
        else:
            columns[z] = proj[0, core] + proj_in[0]
    mixes.wait_recv()

    expert = me // 2
    experts_rows = jnp.concatenate(
        [
            mix_all[a, b, c, pl.ds(expert, 1), :]
            for a in range(zs)
            for b in range(2)
            for c in range(2)
        ],
        axis=0,
    )
    mix_cols[...] = experts_rows.T

    for copy in returns:
        copy.wait_recv()
    mine = pl.ds(pl.multiple_of(core * half, half), half)
    added = jnp.concatenate([columns[a] for a in range(zs)], axis=1)
    stream = x_ref[mine, :].astype(jnp.float32) + added
    kept_rows[...] = stream
    mean_sq = jnp.mean(stream * stream, axis=-1, keepdims=True)
    normed = (stream * lax.rsqrt(mean_sq + EPS) * gain_ref[...]).astype(jnp.bfloat16)
    r = half // 2
    for p in range(2):
        tok[core, p, z, y, x] = normed[p * r : (p + 1) * r]
    across = gather(
        [
            (lambda *at: tok.at[(core, 0, *at)], True),
            (lambda *at: tok.at[(core, 1, *at)], False),
        ]
    )
    def near(ref, side, p):
        return ref.at[side, 0, :, y] if p == 0 else ref.at[side, 1, :, :, x]

    def far(ref, side, p, zt):
        return ref.at[side, 0, zt, 1 - y] if p == 0 else ref.at[side, 1, zt, :, 1 - x]

    def expert_rows(rows_in, scale):
        gate = jnp.dot(rows_in, gu[0], preferred_element_type=jnp.float32)
        upper = jnp.dot(rows_in, gu[1], preferred_element_type=jnp.float32)
        hidden = (upper + 1.0) * gate * jax.nn.sigmoid(1.702 * gate) * scale
        result = jnp.dot(hidden.astype(jnp.bfloat16), dn[...], preferred_element_type=jnp.float32)
        return result.astype(jnp.bfloat16)

    def scales(side, p, places):
        cols = mix_cols[pl.ds(pl.multiple_of(side * half + p * r, r), r), :]
        lane = lax.broadcasted_iota(jnp.int32, cols.shape, 1)
        return [
            jnp.sum(jnp.where(lane == place, cols, 0.0), axis=1, keepdims=True) for place in places
        ]

    def place(zt, yy, xx):
        return zt * 4 + yy * 2 + xx

    over_near = [push(near(tok, core, p), near(tok, core, p), to_core) for p in range(2)]
    load_gu.wait()
    load_dn.wait()

    def run_near(side):
        rows_in, scale = [], []
        for p in range(2):
            rows_in.append(near(tok, side, p)[...].reshape(2 * zs * r, width))
            scale += scales(
                side,
                p,
                [
                    place(a, y, b) if p == 0 else place(a, b, x)
                    for a in range(zs)
                    for b in range(2)
                ],
            )
        result = expert_rows(jnp.concatenate(rows_in, axis=0), jnp.concatenate(scale, axis=0))
        result = result.reshape(2, zs, 2, r, width)
        for p in range(2):
            near(part_out, side, p)[...] = result[p]

    def arrive(d):
        zt = lax.rem(z - d + zs, zs)
        copies = []
        for p in range(2):
            across[p][d].wait_recv()
            across[p][zs + d].wait_recv()
            copies.append(push(far(tok, core, p, zt), far(tok, core, p, zt), to_core))
        return copies

    def run_far(d, copies):
        zt = lax.rem(z - d + zs, zs)
        for copy in copies:
            copy.wait_recv()
        rows_in, scale = [], []
        for side in (core, other):
            for p in range(2):
                rows_in.append(far(tok, side, p, zt)[...].reshape(2 * r, width))
                scale += scales(
                    side,
                    p,
                    [place(zt, 1 - y, b) if p == 0 else place(zt, b, 1 - x) for b in range(2)],
                )
        result = expert_rows(jnp.concatenate(rows_in, axis=0), jnp.concatenate(scale, axis=0))
        result = result.reshape(2, 2, 2, r, width)
        for n, side in enumerate((core, other)):
            for p in range(2):
                far(part_out, side, p, zt)[...] = result[n, p]
        return [
            push(far(part_out, other, p, zt), from_core.at[p, zs + d], to_core) for p in range(2)
        ]

    def add_far(d, copies):
        zt = lax.rem(z - d + zs, zs)
        started = []
        for p in range(2):
            copies[p].wait_recv()
            block = far(part_out, core, p, zt)
            total = block[...].astype(jnp.float32) + from_core[p, zs + d].astype(jnp.float32)
            block[...] = total.astype(jnp.bfloat16)
            started.append(push(block, from_first.at[p, d], to_y if p == 0 else to_x))
        return started

    run_near(core)
    crossed = [arrive(0)]
    for copy in over_near:
        copy.wait_recv()
    run_near(other)
    near_back = [
        push(near(part_out, other, p), from_core.at[p, pl.ds(0, zs)], to_core) for p in range(2)
    ]
    done, firsts = [], []
    for d in range(zs):
        if d + 1 < zs:
            crossed.append(arrive(d + 1))
        done.append(run_far(d, crossed[d]))
        if d:
            firsts.append(add_far(d - 1, done[d - 1]))
    firsts.append(add_far(zs - 1, done[zs - 1]))
    for p in range(2):
        near_back[p].wait_recv()
    seconds, lasts = [[], []], [[], []]
    for d in range(zs):
        for p in range(2):
            zt = lax.rem(z - d + zs, zs)
            firsts[d][p].wait_recv()
            kept = part_out[core, 0, zt, y] if p == 0 else part_out[core, 1, zt, :, x]
            total = kept.astype(jnp.float32) + from_core[p, zt].astype(jnp.float32)
            total = total + from_first[p, d].astype(jnp.float32)
            mid[p, d] = total.astype(jnp.bfloat16)
            away = mid.at[p, d, 1 - (x if p == 0 else y)]
            seconds[p].append(push(away, from_second.at[p, d], to_x if p == 0 else to_y))
    totals = []
    for d in range(zs):
        for p in range(2):
            seconds[p][d].wait_recv()
            kept = mid[p, d, x if p == 0 else y].astype(jnp.float32)
            total = kept + from_second[p, d].astype(jnp.float32)
            if d:
                to_send[p, d - 1] = total.astype(jnp.bfloat16)
                lasts[p].append(push(to_send.at[p, d - 1], from_z.at[p, d - 1], to_z[zs - d]))
            else:
                totals.append(total)
    for p in range(2):
        total = totals[p]
        for e in range(1, zs):
            lasts[p][e - 1].wait_recv()
            total = total + from_z[p, e - 1].astype(jnp.float32)
        out_ref[p * r : (p + 1) * r, :] = (kept_rows[p * r : (p + 1) * r, :] + total).astype(
            jnp.bfloat16
        )
    for copy in sent:
        copy.wait_send()


def fused_path(
    holders,
    x_pre,
    x_dec,
    prefill_query_rows,
    prefill_key_values,
    decode_query_rows,
    decode_key_values,
    cache,
    cache_len,
    sinks,
    o_weight,
    norm_gain,
    expert_ids,
    route_logits,
    w_gate_up,
    w_down,
):
    attn_rows = attention_rows(
        x_pre,
        x_dec,
        prefill_query_rows,
        prefill_key_values,
        decode_query_rows,
        decode_key_values,
        cache,
        cache_len,
        sinks,
    )
    tokens, inner = attn_rows.shape
    width = x_pre.shape[1]
    hidden = w_down.shape[1]
    columns = o_weight.shape[1]
    zs = holders // 4
    half, r = tokens // 2, tokens // 4
    experts = holders // 2
    resid = jnp.concatenate([x_pre, x_dec], axis=0)
    wo = o_weight.reshape(2, inner // 2, columns).transpose(0, 2, 1)
    mix = jax.nn.softmax(route_logits, axis=-1)
    chosen = expert_ids[None, :, :] == jnp.arange(experts, dtype=jnp.int32)[:, None, None]
    blend = jnp.sum(jnp.where(chosen, mix[None], 0.0), axis=-1)
    blend = jnp.pad(blend, ((0, 0), (0, -tokens % 128)))
    bf = jnp.bfloat16
    grid = (zs, 2, 2)
    return pl.pallas_call(
        functools.partial(layer_kernel, zs),
        out_shape=jax.ShapeDtypeStruct((half, width), bf),
        in_specs=[pl.BlockSpec(memory_space=pltpu.VMEM)] * 5
        + [pl.BlockSpec(memory_space=pl.ANY)] * 2,
        out_specs=pl.BlockSpec(memory_space=pltpu.VMEM),
        scratch_shapes=[
            pltpu.VMEM((2, 2, 2, columns, inner // 2), bf),
            pltpu.VMEM((*grid, *blend.shape), jnp.float32),
            pltpu.VMEM((blend.shape[1], holders), jnp.float32),
            pltpu.VMEM((zs - 1, tokens, inner), bf),
            pltpu.VMEM((zs, 2, half, width // zs), jnp.float32),
            pltpu.VMEM((zs, half, width // zs), jnp.float32),
            pltpu.VMEM((zs, half, width // zs), jnp.float32),
            pltpu.VMEM((half, width), jnp.float32),
            pltpu.VMEM((2, 2, *grid, r, width), bf),
            pltpu.VMEM((2, 2, *grid, r, width), bf),
            pltpu.VMEM((2, 2 * zs, 2, r, width), bf),
            pltpu.VMEM((2, zs, 2, r, width), bf),
            pltpu.VMEM((2, zs, 2, r, width), bf),
            pltpu.VMEM((2, zs, r, width), bf),
            pltpu.VMEM((2, zs - 1, r, width), bf),
            pltpu.VMEM((2, zs - 1, r, width), bf),
            pltpu.VMEM((2, width, hidden), bf),
            pltpu.VMEM((hidden, width), bf),
            pltpu.SemaphoreType.DMA((192,)),
            pltpu.SemaphoreType.DMA((192,)),
            pltpu.SemaphoreType.DMA((2,)),
        ],
        compiler_params=pltpu.CompilerParams(
            collective_id=0, has_side_effects=True, vmem_limit_bytes=60 * 2**20
        ),
    )(attn_rows, wo, resid, norm_gain.reshape(1, width), blend, w_gate_up[0], w_down[0])


def on_device(holders, *args):
    x_pre, x_dec, o_weight = args[0], args[1], args[9]
    tokens = x_pre.shape[0] + x_dec.shape[0]
    gathered = 2 * holders * (tokens * x_pre.shape[1] * 4 + o_weight.size)
    if holders % 4 == 0 and holders >= 8 and tokens % 64 == 0 and gathered < 32 * 2**20:
        return fused_path(holders, *args)
    return general_path(*args)


def solution(mesh):
    placed = (
        P(("groups", "ep"), None),
        P(("groups", "ep"), None),
        P(("groups", "ep"), "hp"),
        P(None, ("groups", "ep"), "hp"),
        P(("groups", "ep"), "hp"),
        P(None, ("groups", "ep"), "hp"),
        P(None, ("groups", "ep"), None, "hp"),
        P(("groups", "ep")),
        P("hp"),
        P("hp", "ep"),
        P(),
        P(("groups", "ep"), None),
        P(("groups", "ep"), None),
        P("ep", None, None, "hp"),
        P("ep", "hp", None),
    )
    return jax.shard_map(
        functools.partial(on_device, mesh.shape["ep"]),
        mesh=mesh,
        in_specs=placed,
        out_specs=P(("groups", "ep", "hp"), None),
        check_vma=False,
    )
```
